32 devices in a mesh: dp: 4 (over y, z), tp: 8 (over x, core).
Axes of the slice: x: 4, y: 2, z: 2, core: 2. Of those that a mesh axis runs over, the one named last changes fastest.
The devices are a block of a 4x4x8 slice.
Arguments:
- x_in: bfloat16 [2, 1024, 2048], P(None, ('dp', 'tp')), parts along dimension 1
- y_cot: bfloat16 [2, 1024, 2048], P(None, ('dp', 'tp')), parts along dimension 1
- gain_attn: float32 [2, 2048], replicated
- gain_mlp: float32 [2, 2048], replicated
- w_qkv: bfloat16 [2, 2048, 8, 4, 128], P(None, None, 'tp')
- w_out: bfloat16 [2, 16, 128, 2048], P(None, 'tp')
- w_gate: bfloat16 [2, 2048, 6144], P(None, None, 'tp')
- w_up: bfloat16 [2, 2048, 6144], P(None, None, 'tp')
- w_down: bfloat16 [2, 6144, 2048], P(None, 'tp')
Outputs:
- output 1: bfloat16 [2, 1024, 2048], P(None, ('dp', 'tp')), parts along dimension 1
- output 2: bfloat16 [2, 1024, 2048], P(None, ('dp', 'tp')), parts along dimension 1
- output 3: bfloat16 [8, 2048, 8, 4, 128], P('dp', None, 'tp'), parts along dimension 0
- output 4: bfloat16 [8, 16, 128, 2048], P('dp', 'tp'), parts along dimension 0
- output 5: bfloat16 [8, 2048, 6144], P('dp', None, 'tp'), parts along dimension 0
- output 6: bfloat16 [8, 2048, 6144], P('dp', None, 'tp'), parts along dimension 0
- output 7: bfloat16 [8, 6144, 2048], P('dp', 'tp'), parts along dimension 0
- output 8: float32 [8, 2048], P('dp'), parts along dimension 0
- output 9: float32 [8, 2048], P('dp'), parts along dimension 0
There are 4 independent parts. The reference program is written for one: setup_inputs(seed, part) draws one part's arguments, and reference() takes and returns one part's arrays. A program takes and returns all parts, laid end to end along the dimension named above; an argument that names none is the same for every part.
All inputs are finite; a program needn't handle non-finite values.
Results may differ from the reference program's by a relative error of at most 0.02.
Values are sent between devices in bfloat16 or wider.
A program may use at most 768 MiB of HBM per device.

```python
import jax
import jax.numpy as jnp
from jax import lax

D = 2048
FF = 6144
HEADS = 16
KV_HEADS = 8
HEAD = 128
SEQ = 256
LAYERS = 2
MICRO = 2
GROUP = HEADS // KV_HEADS
NORM_EPS = 1e-5


def setup_inputs(seed: int = 0, part: int = 0) -> dict:
    base_key = jax.random.key(seed)
    shared_keys = jax.random.split(base_key, 7)
    part_keys = jax.random.split(jax.random.fold_in(base_key, part), 2)
    x_in = jax.random.normal(part_keys[0], (MICRO, SEQ, D), jnp.float32)
    y_cot = jax.random.normal(part_keys[1], (MICRO, SEQ, D), jnp.float32)
    gain_attn = 1.0 + 0.3 * jax.random.normal(shared_keys[0], (LAYERS, D), jnp.float32)
    gain_mlp = 1.0 + 0.3 * jax.random.normal(shared_keys[1], (LAYERS, D), jnp.float32)
    w_qkv = jax.random.normal(shared_keys[2], (LAYERS, D, KV_HEADS, GROUP + 2, HEAD), jnp.float32) * D ** -0.5
    w_out = jax.random.normal(shared_keys[3], (LAYERS, HEADS, HEAD, D), jnp.float32) * (HEADS * HEAD) ** -0.5
    w_gate = jax.random.normal(shared_keys[4], (LAYERS, D, FF), jnp.float32) * D ** -0.5
    w_up = jax.random.normal(shared_keys[5], (LAYERS, D, FF), jnp.float32) * D ** -0.5
    w_down = jax.random.normal(shared_keys[6], (LAYERS, FF, D), jnp.float32) * FF ** -0.5
    return {'x_in': x_in.astype(jnp.bfloat16), 'y_cot': y_cot.astype(jnp.bfloat16), 'gain_attn': gain_attn, 'gain_mlp': gain_mlp, 'w_qkv': w_qkv.astype(jnp.bfloat16), 'w_out': w_out.astype(jnp.bfloat16), 'w_gate': w_gate.astype(jnp.bfloat16), 'w_up': w_up.astype(jnp.bfloat16), 'w_down': w_down.astype(jnp.bfloat16)}


def rms_norm(row_vals, gain_vec):
    return row_vals * lax.rsqrt(jnp.mean(row_vals * row_vals, axis=-1, keepdims=True) + NORM_EPS) * gain_vec


def group_attention(queries, key_rows, value_rows):
    scores = jnp.einsum('qge,ke->gqk', queries.astype(jnp.float32), key_rows.astype(jnp.float32)) * HEAD ** -0.5
    positions = jnp.arange(SEQ)
    scores = jnp.where(positions[:, None] >= positions[None, :], scores, -1e30)
    prob_b16 = jax.nn.softmax(scores, axis=-1).astype(jnp.bfloat16)
    attn_mix = jnp.einsum('gqk,ke->qge', prob_b16.astype(jnp.float32), value_rows.astype(jnp.float32))
    return attn_mix.astype(jnp.bfloat16)


attention_ckpt = jax.checkpoint(group_attention)


def group_step(group_args):
    return attention_ckpt(group_args[0], group_args[1], group_args[2])


def layer_forward(layer_in, layer_params):
    gain_first, gain_second, qkv_weight, out_weight, gate_weight, up_weight, down_weight = layer_params
    x_f32 = layer_in.astype(jnp.float32)
    normed = rms_norm(x_f32, gain_first).astype(jnp.bfloat16)
    qkv_heads = jnp.einsum('sd,dkje->skje', normed.astype(jnp.float32), qkv_weight).astype(jnp.bfloat16)
    attn_mix = lax.map(group_step, (jnp.swapaxes(qkv_heads[:, :, :GROUP], 0, 1), jnp.swapaxes(qkv_heads[:, :, GROUP], 0, 1), jnp.swapaxes(qkv_heads[:, :, GROUP + 1], 0, 1)))
    attn_sum = jnp.einsum('kqge,kged->qd', attn_mix.astype(jnp.float32), out_weight.reshape(KV_HEADS, GROUP, HEAD, D))
    hidden = (x_f32 + attn_sum.astype(jnp.bfloat16).astype(jnp.float32)).astype(jnp.bfloat16)
    normed_b = rms_norm(hidden.astype(jnp.float32), gain_second).astype(jnp.bfloat16)
    gate_pre = jnp.dot(normed_b.astype(jnp.float32), gate_weight, preferred_element_type=jnp.float32)
    up_proj = jnp.dot(normed_b.astype(jnp.float32), up_weight, preferred_element_type=jnp.float32)
    inner = (jax.nn.silu(gate_pre) * up_proj).astype(jnp.bfloat16)
    down_sum = jnp.dot(inner.astype(jnp.float32), down_weight, preferred_element_type=jnp.float32).astype(jnp.bfloat16)
    return (hidden.astype(jnp.float32) + down_sum.astype(jnp.float32)).astype(jnp.bfloat16)


def stack_forward(layer_in, params):
    def layer_body(carry, layer_params):
        return layer_forward(carry, layer_params), None
    final_rows, unused = lax.scan(layer_body, layer_in, params)
    return final_rows


def reference(x_in, y_cot, gain_attn, gain_mlp, w_qkv, w_out, w_gate, w_up, w_down):
    params = (gain_attn, gain_mlp, w_qkv.astype(jnp.float32), w_out.astype(jnp.float32), w_gate.astype(jnp.float32), w_up.astype(jnp.float32), w_down.astype(jnp.float32))
    first_out, first_pull = jax.vjp(stack_forward, x_in[0], params)
    first_rows, first_grads = first_pull(y_cot[0])
    second_out, second_pull = jax.vjp(stack_forward, x_in[1], params)
    second_rows, second_grads = second_pull(y_cot[1])
    summed = [grad_one + grad_two for grad_one, grad_two in zip(first_grads, second_grads)]
    return (jnp.stack([first_out, second_out]), jnp.stack([first_rows, second_rows]), summed[2].astype(jnp.bfloat16), summed[3].astype(jnp.bfloat16), summed[4].astype(jnp.bfloat16), summed[5].astype(jnp.bfloat16), summed[6].astype(jnp.bfloat16), summed[0], summed[1])
```

```python
import functools

import jax
import jax.numpy as jnp
from jax import lax
from jax.experimental import pallas as pl
from jax.experimental.pallas import tpu as pltpu
from jax.sharding import PartitionSpec as P

NORM_EPS = 1e-5
F32 = jnp.float32
BF16 = jnp.bfloat16
MESH = pl.DeviceIdType.MESH
ANY = pl.BlockSpec(memory_space=pl.ANY)
VMEM = pl.BlockSpec(memory_space=pltpu.VMEM)
AG_COPIES = 11
RS_COPIES = 10
NN = (((1,), (0,)), ((), ()))
NT = (((1,), (1,)), ((), ()))
TN = (((0,), (0,)), ((), ()))


def dot(a, b, dims=NN):
    return lax.dot_general(a, b, dims, preferred_element_type=F32)


def aligned(index, size):
    return pl.ds(pl.multiple_of(index * size, size), size)


class Ring:
    def __init__(self, devices, rows, send_sems, recv_sems):
        self.chips = devices // 2
        self.rows = rows
        self.send_sems, self.recv_sems = send_sems, recv_sems
        self.used = 0
        self.me = lax.axis_index('tp')
        self.chip = self.me // 2
        self.core = self.me % 2
        self.right_chip = lax.rem(self.chip + 1, self.chips)
        self.left_chip = lax.rem(self.chip + self.chips - 1, self.chips)
        self.far_chip = lax.rem(self.chip + 2, self.chips)
        self.right = self.right_chip * 2 + self.core
        self.left = self.left_chip * 2 + self.core
        self.far = self.far_chip * 2 + self.core
        self.partner = self.chip * 2 + 1 - self.core
        self.peers = (self.left, self.right, self.partner)

    def greet(self):
        barrier = pltpu.get_barrier_semaphore()
        for peer in self.peers:
            pl.semaphore_signal(barrier, inc=1, device_id={'tp': peer}, device_id_type=MESH)
        pl.semaphore_wait(barrier, len(self.peers))

    def send(self, src, dst, device):
        copy = pltpu.make_async_remote_copy(src, dst, self.send_sems.at[self.used], self.recv_sems.at[self.used],
                                            device_id={'tp': device}, device_id_type=MESH)
        self.used += 1
        copy.start()
        return copy


class Gather:
    def __init__(self, ring, full):
        self.ring, self.full = ring, full
        self.half = ring.rows // 2

    def block(self, owner):
        return self.full.at[aligned(owner, self.ring.rows)]

    def part(self, owner, index):
        return self.full.at[pl.ds(pl.multiple_of(owner * self.ring.rows + index * self.half, self.half), self.half)]

    def start(self):
        ring = self.ring
        low, high, whole = self.part(ring.me, 0), self.part(ring.me, 1), self.block(ring.me)
        self.r0 = ring.send(low, low, ring.right)
        self.l1 = ring.send(high, high, ring.left)
        self.r1 = ring.send(high, high, ring.right)
        self.l0 = ring.send(low, low, ring.left)
        self.own = ring.send(whole, whole, ring.partner)

    def relay(self):
        ring = self.ring
        from_left, from_right = self.part(ring.left, 0), self.part(ring.right, 1)
        self.r0.wait_recv()
        self.relay_r = ring.send(from_left, from_left, ring.right)
        self.l1.wait_recv()
        self.relay_l = ring.send(from_right, from_right, ring.left)
        self.r1.wait_recv()
        left_block = self.block(ring.left)
        self.pass_left = ring.send(left_block, left_block, ring.partner)
        self.l0.wait_recv()
        right_block = self.block(ring.right)
        self.pass_right = ring.send(right_block, right_block, ring.partner)

    def finish(self):
        ring = self.ring
        far_low, far_high = self.part(ring.far, 0), self.part(ring.far, 1)
        self.relay_r.wait_recv()
        self.pass_low = ring.send(far_low, far_low, ring.partner)
        self.relay_l.wait_recv()
        self.pass_high = ring.send(far_high, far_high, ring.partner)
        for copy in (self.own, self.pass_left, self.pass_right, self.pass_low, self.pass_high):
            copy.wait_recv()

    def sent(self):
        for copy in (self.r0, self.l1, self.r1, self.l0, self.own, self.relay_r, self.relay_l, self.pass_left,
                     self.pass_right, self.pass_low, self.pass_high):
            copy.wait_send()


class Reduce:
    def __init__(self, ring, part, bufs):
        self.ring, self.part = ring, part
        self.from_partner, self.sums, self.via_left, self.via_right, self.in_left, self.in_right = bufs
        self.half = ring.rows // 2
        self.chips = (ring.far_chip, ring.right_chip, ring.left_chip, ring.chip)

    def start(self):
        ring = self.ring
        self.swaps = []
        for slot, chip in enumerate(self.chips):
            rows = self.part.at[aligned(chip * 2 + 1 - ring.core, ring.rows)]
            self.swaps.append(ring.send(rows, self.from_partner.at[slot], ring.partner))

    def add(self, slot):
        self.swaps[slot].wait_recv()
        rows = aligned(self.chips[slot] * 2 + self.ring.core, self.ring.rows)
        self.sums[slot] = self.part[rows, :] + self.from_partner[slot]

    def far_out(self):
        ring, half = self.ring, self.half
        self.add(0)
        self.far_r = ring.send(self.sums.at[0, 0:half], self.via_left, ring.right)
        self.far_l = ring.send(self.sums.at[0, half:2 * half], self.via_right, ring.left)

    def near_out(self):
        ring, half = self.ring, self.half
        self.add(1)
        self.near_r = ring.send(self.sums.at[1, half:2 * half], self.in_left.at[half:2 * half], ring.right)
        self.add(2)
        self.near_l = ring.send(self.sums.at[2, 0:half], self.in_right.at[0:half], ring.left)
        self.add(3)

    def relay(self):
        ring, half = self.ring, self.half
        self.far_r.wait_recv()
        self.sums[1, 0:half] = self.sums[1, 0:half] + self.via_left[...]
        self.relay_r = ring.send(self.sums.at[1, 0:half], self.in_left.at[0:half], ring.right)
        self.far_l.wait_recv()
        self.sums[2, half:2 * half] = self.sums[2, half:2 * half] + self.via_right[...]
        self.relay_l = ring.send(self.sums.at[2, half:2 * half], self.in_right.at[half:2 * half], ring.left)

    def finish(self):
        for copy in (self.near_r, self.near_l, self.relay_r, self.relay_l):
            copy.wait_recv()
        return self.sums[3] + self.in_left[...] + self.in_right[...]

    def sent(self):
        for copy in (*self.swaps, self.far_r, self.far_l, self.near_r, self.near_l, self.relay_r, self.relay_l):
            copy.wait_send()


def reduce_scratch(rows, width):
    return [pltpu.VMEM((4, rows, width), F32), pltpu.VMEM((4, rows, width), F32),
            pltpu.VMEM((rows // 2, width), F32), pltpu.VMEM((rows // 2, width), F32),
            pltpu.VMEM((rows, width), F32), pltpu.VMEM((rows, width), F32)]


REDUCE_BUFS = 6


def norm_rows(row_vals, gain_vec):
    vals = row_vals.astype(F32)
    return (vals * lax.rsqrt(jnp.mean(vals * vals, axis=-1, keepdims=True) + NORM_EPS) * gain_vec).astype(BF16)


def norm_rows_backward(row_vals, gain_vec, cot_rows):
    vals = row_vals.astype(F32)
    scale = lax.rsqrt(jnp.mean(vals * vals, axis=-1, keepdims=True) + NORM_EPS)
    unit = vals * scale
    grad_gain = jnp.sum(cot_rows * unit, axis=0, keepdims=True)
    cot_unit = cot_rows * gain_vec
    grad_vals = scale * (cot_unit - unit * jnp.mean(cot_unit * unit, axis=-1, keepdims=True))
    return grad_vals, grad_gain


def head_probs(query, key, score_scale):
    seq_len = query.shape[0]
    scores = dot(query, key, NT) * score_scale
    row_pos = lax.broadcasted_iota(jnp.int32, (seq_len, seq_len), 0)
    col_pos = lax.broadcasted_iota(jnp.int32, (seq_len, seq_len), 1)
    scores = jnp.where(row_pos >= col_pos, scores, -1e30)
    exp_scores = jnp.exp(scores - jnp.max(scores, axis=-1, keepdims=True))
    return exp_scores / jnp.sum(exp_scores, axis=-1, keepdims=True)


def credit_signal(ring, credit):
    for peer in ring.peers:
        pl.semaphore_signal(credit, inc=1, device_id={'tp': peer}, device_id_type=MESH)


def residual(row_vals, total):
    return (row_vals.astype(F32) + total.astype(BF16).astype(F32)).astype(BF16)


def forward_skeleton(ring, rows_ref, gain, out_ref, full, credit, reducers, ready, gathered, partial):
    own = aligned(ring.me, ring.rows)
    ring.greet()
    full[own, :] = norm_rows(rows_ref[0], gain)
    first = Gather(ring, full)
    first.start()
    first.relay()
    first.finish()
    ready()
    gathered(0)
    first.sent()
    credit_signal(ring, credit)
    pl.semaphore_wait(credit, len(ring.peers))
    full[own, :] = norm_rows(rows_ref[1], gain)
    second = Gather(ring, full)
    second.start()
    partial(0)
    reducers[0].start()
    reducers[0].far_out()
    reducers[0].near_out()
    second.relay()
    second.finish()
    gathered(1)
    reducers[0].relay()
    partial(1)
    reducers[1].start()
    reducers[1].far_out()
    reducers[1].near_out()
    out_ref[0] = residual(rows_ref[0], reducers[0].finish())
    reducers[1].relay()
    out_ref[1] = residual(rows_ref[1], reducers[1].finish())
    second.sent()
    reducers[0].sent()
    reducers[1].sent()


def loop_columns(count, body):
    def step(index, carry):
        body(index)
        return carry
    lax.fori_loop(0, count, step, 0)


def attention_forward_kernel(layer, devices, head_dim, groups, rows_ref, gain_ref, w_qkv, w_out, out_ref, qkv_ref, mix_ref,
                             qkv_w, out_w, full, part_a, part_b, *rest):
    bufs_a, bufs_b = rest[:REDUCE_BUFS], rest[REDUCE_BUFS:2 * REDUCE_BUFS]
    load_sem, send_sems, recv_sems, credit = rest[2 * REDUCE_BUFS:]
    ring = Ring(devices, rows_ref.shape[1], send_sems, recv_sems)
    loads = [pltpu.make_async_copy(w_qkv.at[layer], qkv_w, load_sem.at[0]),
             pltpu.make_async_copy(w_out.at[layer], out_w, load_sem.at[1])]
    for load in loads:
        load.start()
    parts = (part_a, part_b)
    reducers = [Reduce(ring, part_a, bufs_a), Reduce(ring, part_b, bufs_b)]

    def ready():
        for load in loads:
            load.wait()

    def gathered(micro):
        qkv_ref[micro] = dot(full[...], qkv_w[...]).astype(BF16)

    def partial(micro):
        key = qkv_ref[micro, :, groups * head_dim:(groups + 1) * head_dim]
        value = qkv_ref[micro, :, (groups + 1) * head_dim:]
        for head in range(groups):
            cols = slice(head * head_dim, (head + 1) * head_dim)
            prob = head_probs(qkv_ref[micro, :, cols], key, head_dim ** -0.5).astype(BF16)
            mix_ref[micro, :, cols] = dot(prob, value).astype(BF16)

        def columns(index):
            cols = aligned(index, 512)
            parts[micro][:, cols] = dot(mix_ref[micro], out_w[:, cols])
        loop_columns(out_w.shape[1] // 512, columns)

    forward_skeleton(ring, rows_ref, gain_ref[layer:layer + 1, :], out_ref, full, credit, reducers, ready, gathered, partial)


def mlp_forward_kernel(layer, devices, rows_ref, gain_ref, w_gate, w_up, w_down, out_ref,
                       gate_w, up_w, down_w, inner, full, part_a, part_b, *rest):
    bufs_a, bufs_b = rest[:REDUCE_BUFS], rest[REDUCE_BUFS:2 * REDUCE_BUFS]
    load_sem, send_sems, recv_sems, credit = rest[2 * REDUCE_BUFS:]
    ring = Ring(devices, rows_ref.shape[1], send_sems, recv_sems)
    loads = [pltpu.make_async_copy(src.at[layer], dst, load_sem.at[index])
             for index, (src, dst) in enumerate(((w_gate, gate_w), (w_up, up_w), (w_down, down_w)))]
    for load in loads:
        load.start()
    parts = (part_a, part_b)
    reducers = [Reduce(ring, part_a, bufs_a), Reduce(ring, part_b, bufs_b)]

    def ready():
        for load in loads:
            load.wait()

    def gathered(micro):
        def columns(index):
            cols = aligned(index, 256)
            gate_pre = dot(full[...], gate_w[:, cols])
            up_proj = dot(full[...], up_w[:, cols])
            inner[:, cols] = (gate_pre * jax.nn.sigmoid(gate_pre) * up_proj).astype(BF16)
        loop_columns(gate_w.shape[1] // 256, columns)

    def partial(micro):
        def columns(index):
            cols = aligned(index, 512)
            parts[micro][:, cols] = dot(inner[...], down_w[:, cols])
        loop_columns(down_w.shape[1] // 512, columns)

    forward_skeleton(ring, rows_ref, gain_ref[layer:layer + 1, :], out_ref, full, credit, reducers, ready, gathered, partial)


def backward_skeleton(ring, rows_ref, cot_ref, gain, out_ref, grad_gain_ref, full, cots, credit, reducers, ready,
                      partial, weights_near, weights_far, weights_out):
    own = aligned(ring.me, ring.rows)
    ring.greet()
    full[own, :] = norm_rows(rows_ref[0], gain)
    first = Gather(ring, full)
    first.start()
    for micro in range(2):
        cots[micro, own, :] = cot_ref[micro]
    cot_gathers = [Gather(ring, cots.at[micro]) for micro in range(2)]
    cot_gathers[0].start()
    first.relay()
    first.finish()
    cot_gathers[0].relay()
    cot_gathers[1].start()
    cot_gathers[0].finish()
    ready()
    partial(0)
    reducers[0].start()
    reducers[0].far_out()
    reducers[0].near_out()
    weights_near(0)
    first.sent()
    credit_signal(ring, credit)
    cot_gathers[1].relay()
    reducers[0].relay()
    cot_gathers[1].finish()
    pl.semaphore_wait(credit, len(ring.peers))
    full[own, :] = norm_rows(rows_ref[1], gain)
    second = Gather(ring, full)
    second.start()
    weights_far(0)
    second.relay()
    second.finish()
    partial(1)
    reducers[1].start()
    reducers[1].far_out()
    reducers[1].near_out()
    total = reducers[0].finish().astype(BF16).astype(F32)
    grad_rows, grad_gain_0 = norm_rows_backward(rows_ref[0], gain, total)
    out_ref[0] = (cot_ref[0].astype(F32) + grad_rows).astype(BF16)
    weights_near(1)
    reducers[1].relay()
    weights_far(1)
    weights_out()
    total = reducers[1].finish().astype(BF16).astype(F32)
    grad_rows, grad_gain_1 = norm_rows_backward(rows_ref[1], gain, total)
    out_ref[1] = (cot_ref[1].astype(F32) + grad_rows).astype(BF16)
    grad_gain_ref[...] = grad_gain_0 + grad_gain_1
    second.sent()
    for micro in range(2):
        cot_gathers[micro].sent()
        reducers[micro].sent()


def mlp_backward_kernel(layer, devices, rows_ref, cot_ref, gain_ref, w_gate, w_up, w_down,
                        out_ref, grad_gain_ref, grad_gate_out, grad_up_out, grad_down_out,
                        gate_w, up_w, down_w, inner, grad_gate, grad_up, acc_gate, acc_up, acc_down,
                        stage_gate, stage_up, stage_down, full, cots, part_a, part_b, *rest):
    bufs_a, bufs_b = rest[:REDUCE_BUFS], rest[REDUCE_BUFS:2 * REDUCE_BUFS]
    load_sem, store_sem, send_sems, recv_sems, credit = rest[2 * REDUCE_BUFS:]
    ring = Ring(devices, rows_ref.shape[1], send_sems, recv_sems)
    loads = [pltpu.make_async_copy(src.at[layer], dst, load_sem.at[index])
             for index, (src, dst) in enumerate(((w_gate, gate_w), (w_up, up_w), (w_down, down_w)))]
    for load in loads:
        load.start()
    parts = (part_a, part_b)
    reducers = [Reduce(ring, part_a, bufs_a), Reduce(ring, part_b, bufs_b)]
    stores = [pltpu.make_async_copy(src, dst, store_sem.at[index]) for index, (src, dst) in enumerate(
        ((stage_gate, grad_gate_out), (stage_up, grad_up_out), (stage_down, grad_down_out)))]

    def ready():
        for load in loads:
            load.wait()

    def partial(micro):
        def columns(index):
            cols = aligned(index, 256)
            gate_pre = dot(full[...], gate_w[:, cols])
            up_proj = dot(full[...], up_w[:, cols])
            grad_inner = dot(cots[micro], down_w[cols, :], NT).astype(BF16).astype(F32)
            gate_sig = jax.nn.sigmoid(gate_pre)
            gate_act = gate_pre * gate_sig
            inner[:, cols] = (gate_act * up_proj).astype(BF16)
            grad_up[:, cols] = (grad_inner * gate_act).astype(BF16)
            grad_gate[:, cols] = (grad_inner * up_proj * gate_sig * (1.0 + gate_pre * (1.0 - gate_sig))).astype(BF16)
        loop_columns(gate_w.shape[1] // 256, columns)

        def out_columns(index):
            cols = aligned(index, 256)
            parts[micro][:, cols] = dot(grad_gate[...], gate_w[cols, :], NT) + dot(grad_up[...], up_w[cols, :], NT)
        loop_columns(gate_w.shape[0] // 256, out_columns)

    def put(micro, acc, stage, rows, term):
        if micro == 0:
            acc[rows, :] = term
        else:
            stage[rows, :] = (acc[rows, :] + term).astype(BF16)

    def weights_near(micro):
        def columns(index):
            cols = aligned(index, 256)
            put(micro, acc_gate, stage_gate, cols, dot(full[:, cols], grad_gate[...], TN))
            put(micro, acc_up, stage_up, cols, dot(full[:, cols], grad_up[...], TN))
        loop_columns(full.shape[1] // 256, columns)
        if micro == 1:
            stores[0].start()
            stores[1].start()

    def weights_far(micro):
        def columns(index):
            cols = aligned(index, 128)
            put(micro, acc_down, stage_down, cols, dot(inner[:, cols], cots[micro], TN))
        loop_columns(inner.shape[1] // 128, columns)
        if micro == 1:
            stores[2].start()

    def weights_out():
        for store in stores:
            store.wait()

    backward_skeleton(ring, rows_ref, cot_ref, gain_ref[layer:layer + 1, :], out_ref, grad_gain_ref, full, cots, credit,
                      reducers, ready, partial, weights_near, weights_far, weights_out)


def attention_backward_kernel(layer, devices, head_dim, groups, rows_ref, cot_ref, gain_ref, qkv_ref, mix_ref, w_qkv, w_out,
                              out_ref, grad_gain_ref, grad_qkv_out, grad_out_out,
                              qkv_w, out_w, grad_mix, grad_qkv, acc_qkv, acc_out, stage_qkv, stage_out,
                              full, cots, part_a, part_b, *rest):
    bufs_a, bufs_b = rest[:REDUCE_BUFS], rest[REDUCE_BUFS:2 * REDUCE_BUFS]
    load_sem, store_sem, send_sems, recv_sems, credit = rest[2 * REDUCE_BUFS:]
    ring = Ring(devices, rows_ref.shape[1], send_sems, recv_sems)
    loads = [pltpu.make_async_copy(w_qkv.at[layer], qkv_w, load_sem.at[0]),
             pltpu.make_async_copy(w_out.at[layer], out_w, load_sem.at[1])]
    for load in loads:
        load.start()
    parts = (part_a, part_b)
    reducers = [Reduce(ring, part_a, bufs_a), Reduce(ring, part_b, bufs_b)]
    stores = [pltpu.make_async_copy(stage_qkv, grad_qkv_out, store_sem.at[0]),
              pltpu.make_async_copy(stage_out, grad_out_out, store_sem.at[1])]

    def ready():
        for load in loads:
            load.wait()

    def partial(micro):
        grad_mix[...] = dot(cots[micro], out_w[...], NT).astype(BF16)
        score_scale = head_dim ** -0.5
        key = qkv_ref[micro, :, groups * head_dim:(groups + 1) * head_dim]
        value = qkv_ref[micro, :, (groups + 1) * head_dim:]
        grad_key = grad_value = None
        for head in range(groups):
            cols = slice(head * head_dim, (head + 1) * head_dim)
            query = qkv_ref[micro, :, cols]
            head_grad = grad_mix[:, cols]
            prob = head_probs(query, key, score_scale)
            grad_prob = dot(head_grad, value, NT).astype(BF16).astype(F32)
            row_dot = jnp.sum(grad_prob * prob, axis=-1, keepdims=True)
            grad_scores = (prob * (grad_prob - row_dot) * score_scale).astype(BF16)
            grad_qkv[:, cols] = dot(grad_scores, key).astype(BF16)
            key_term = dot(grad_scores, query, TN)
            value_term = dot(prob.astype(BF16), head_grad, TN)
            grad_key = key_term if grad_key is None else grad_key + key_term
            grad_value = value_term if grad_value is None else grad_value + value_term
        grad_qkv[:, groups * head_dim:(groups + 1) * head_dim] = grad_key.astype(BF16)
        grad_qkv[:, (groups + 1) * head_dim:] = grad_value.astype(BF16)

        def columns(index):
            cols = aligned(index, 256)
            parts[micro][:, cols] = dot(grad_qkv[...], qkv_w[cols, :], NT)
        loop_columns(qkv_w.shape[0] // 256, columns)

    def put(micro, acc, stage, rows, term):
        if micro == 0:
            acc[rows, :] = term
        else:
            stage[rows, :] = (acc[rows, :] + term).astype(BF16)

    def weights_near(micro):
        def columns(index):
            cols = aligned(index, 256)
            put(micro, acc_qkv, stage_qkv, cols, dot(full[:, cols], grad_qkv[...], TN))
        loop_columns(full.shape[1] // 256, columns)
        if micro == 1:
            stores[0].start()

    def weights_far(micro):
        def columns(index):
            cols = aligned(index, 128)
            put(micro, acc_out, stage_out, cols, dot(mix_ref[micro, :, cols], cots[micro], TN))
        loop_columns(mix_ref.shape[2] // 128, columns)
        if micro == 1:
            stores[1].start()

    def weights_out():
        for store in stores:
            store.wait()

    backward_skeleton(ring, rows_ref, cot_ref, gain_ref[layer:layer + 1, :], out_ref, grad_gain_ref, full, cots, credit,
                      reducers, ready, partial, weights_near, weights_far, weights_out)


def gain_sum_kernel(devices, part_ref, out_ref, held, send_sems, recv_sems):
    me = lax.axis_index('tp')
    barrier = pltpu.get_barrier_semaphore()
    others = [lax.rem(me + step, devices) for step in range(1, devices)]
    for peer in others:
        pl.semaphore_signal(barrier, inc=1, device_id={'tp': peer}, device_id_type=MESH)
    pl.semaphore_wait(barrier, len(others))
    copies = []
    for index, peer in enumerate(others):
        copy = pltpu.make_async_remote_copy(part_ref, held.at[me], send_sems.at[index], recv_sems.at[index],
                                            device_id={'tp': peer}, device_id_type=MESH)
        copy.start()
        copies.append(copy)
    held[me] = part_ref[...]
    for copy in copies:
        copy.wait()
    total = held[0]
    for index in range(1, devices):
        total = total + held[index]
    out_ref[...] = total


def comm_params(collective_id):
    return pltpu.CompilerParams(collective_id=collective_id, has_side_effects=True, vmem_limit_bytes=64_000_000)


def solution(mesh):
    devices = mesh.shape['tp']
    row_spec = P(None, ('dp', 'tp'), None)
    gain_spec = P(None, None)
    qkv_spec = P(None, None, 'tp', None, None)
    head_spec = P(None, 'tp', None, None)
    col_spec = P(None, None, 'tp')
    row_shard_spec = P(None, 'tp', None)

    def device_program(x_in, y_cot, gain_attn, gain_mlp, w_qkv, w_out, w_gate, w_up, w_down):
        micro_count, rows, width = x_in.shape
        layer_count = w_qkv.shape[0]
        groups = w_qkv.shape[3] - 2
        head_dim = w_qkv.shape[4]
        seq_len = rows * devices
        qkv_width = (groups + 2) * head_dim
        mix_width = groups * head_dim
        inner_width = w_gate.shape[2]
        w_qkv_flat = w_qkv.reshape(layer_count, width, qkv_width)
        w_out_flat = w_out.reshape(layer_count, mix_width, width)
        row_shape = jax.ShapeDtypeStruct(x_in.shape, BF16)
        gain_shape = jax.ShapeDtypeStruct((1, width), F32)

        def bf16(*shape):
            return pltpu.VMEM(shape, BF16)

        def f32(*shape):
            return pltpu.VMEM(shape, F32)

        def sems(gathers):
            count = gathers * AG_COPIES + 2 * RS_COPIES
            return [pltpu.SemaphoreType.DMA((count,)), pltpu.SemaphoreType.DMA((count,)), pltpu.SemaphoreType.REGULAR]

        full = bf16(seq_len, width)
        reduce_bufs = [f32(seq_len, width), f32(seq_len, width)] + reduce_scratch(rows, width) + reduce_scratch(rows, width)
        attn_weights = [bf16(width, qkv_width), bf16(mix_width, width)]
        mlp_weights = [bf16(width, inner_width), bf16(width, inner_width), bf16(inner_width, width)]

        layer_rows, hidden_rows, qkv_kept, mix_kept = [], [], [], []
        layer_in = x_in
        for layer in range(layer_count):
            layer_rows.append(layer_in)
            hidden, qkv_heads, mix = pl.pallas_call(
                functools.partial(attention_forward_kernel, layer, devices, head_dim, groups),
                out_shape=(row_shape, jax.ShapeDtypeStruct((micro_count, seq_len, qkv_width), BF16),
                           jax.ShapeDtypeStruct((micro_count, seq_len, mix_width), BF16)),
                in_specs=[VMEM, VMEM, ANY, ANY], out_specs=(VMEM, VMEM, VMEM),
                scratch_shapes=attn_weights + [full] + reduce_bufs + [pltpu.SemaphoreType.DMA((2,))] + sems(2),
                compiler_params=comm_params(4 * layer), name=f'attn_fwd_{layer}',
            )(layer_in, gain_attn, w_qkv_flat, w_out_flat)
            qkv_kept.append(qkv_heads)
            mix_kept.append(mix)
            hidden_rows.append(hidden)
            layer_in = pl.pallas_call(
                functools.partial(mlp_forward_kernel, layer, devices),
                out_shape=row_shape, in_specs=[VMEM, VMEM, ANY, ANY, ANY], out_specs=VMEM,
                scratch_shapes=mlp_weights + [bf16(seq_len, inner_width), full] + reduce_bufs
                + [pltpu.SemaphoreType.DMA((3,))] + sems(2),
                compiler_params=comm_params(4 * layer + 1), name=f'mlp_fwd_{layer}',
            )(hidden, gain_mlp, w_gate, w_up, w_down)
        y_rows = layer_in

        grads = [[None] * layer_count for unused in range(5)]
        gain_a, gain_b = [None] * layer_count, [None] * layer_count
        cots = bf16(2, seq_len, width)
        grad_in = y_cot
        for layer in reversed(range(layer_count)):
            grad_hidden, gain_b[layer], grads[2][layer], grads[3][layer], grads[4][layer] = pl.pallas_call(
                functools.partial(mlp_backward_kernel, layer, devices),
                out_shape=(row_shape, gain_shape, jax.ShapeDtypeStruct((width, inner_width), BF16),
                           jax.ShapeDtypeStruct((width, inner_width), BF16), jax.ShapeDtypeStruct((inner_width, width), BF16)),
                in_specs=[VMEM, VMEM, VMEM, ANY, ANY, ANY], out_specs=(VMEM, VMEM, ANY, ANY, ANY),
                scratch_shapes=mlp_weights + [bf16(seq_len, inner_width)] * 3
                + [f32(width, inner_width), f32(width, inner_width), f32(inner_width, width)]
                + mlp_weights + [full, cots] + reduce_bufs
                + [pltpu.SemaphoreType.DMA((3,)), pltpu.SemaphoreType.DMA((3,))] + sems(4),
                compiler_params=comm_params(4 * layer + 2), name=f'mlp_bwd_{layer}',
            )(hidden_rows[layer], grad_in, gain_mlp, w_gate, w_up, w_down)
            grad_in, gain_a[layer], grads[0][layer], grads[1][layer] = pl.pallas_call(
                functools.partial(attention_backward_kernel, layer, devices, head_dim, groups),
                out_shape=(row_shape, gain_shape, jax.ShapeDtypeStruct((width, qkv_width), BF16),
                           jax.ShapeDtypeStruct((mix_width, width), BF16)),
                in_specs=[VMEM, VMEM, VMEM, VMEM, VMEM, ANY, ANY], out_specs=(VMEM, VMEM, ANY, ANY),
                scratch_shapes=attn_weights + [bf16(seq_len, mix_width), bf16(seq_len, qkv_width)]
                + [f32(width, qkv_width), f32(mix_width, width)] + attn_weights + [full, cots] + reduce_bufs
                + [pltpu.SemaphoreType.DMA((2,)), pltpu.SemaphoreType.DMA((2,))] + sems(4),
                compiler_params=comm_params(4 * layer + 3), name=f'attn_bwd_{layer}',
            )(layer_rows[layer], grad_hidden, gain_attn, qkv_kept[layer], mix_kept[layer], w_qkv_flat, w_out_flat)

        gain_part = jnp.concatenate(gain_a + gain_b, axis=0)
        gain_sum = pl.pallas_call(
            functools.partial(gain_sum_kernel, devices),
            out_shape=jax.ShapeDtypeStruct(gain_part.shape, F32), in_specs=[VMEM], out_specs=VMEM,
            scratch_shapes=[pltpu.VMEM((devices, *gain_part.shape), F32), pltpu.SemaphoreType.DMA((devices - 1,)),
                            pltpu.SemaphoreType.DMA((devices - 1,))],
            compiler_params=comm_params(4 * layer_count), name='gain_sum',
        )(gain_part)
        return (y_rows, grad_in,
                jnp.stack(grads[0]).reshape(w_qkv.shape), jnp.stack(grads[1]).reshape(w_out.shape),
                jnp.stack(grads[2]), jnp.stack(grads[3]), jnp.stack(grads[4]),
                gain_sum[:layer_count], gain_sum[layer_count:])

    return jax.shard_map(device_program, mesh=mesh,
                         in_specs=(row_spec, row_spec, gain_spec, gain_spec, qkv_spec, head_spec, col_spec, col_spec, row_shard_spec),
                         out_specs=(row_spec, row_spec, P('dp', None, 'tp', None, None), P('dp', 'tp', None, None), P('dp', None, 'tp'), P('dp', None, 'tp'), P('dp', 'tp', None), P('dp', None), P('dp', None)),
                         check_vma=False)
```

```python
import functools

import jax
import jax.numpy as jnp
from jax import lax
from jax.experimental import pallas as pl
from jax.experimental.pallas import tpu as pltpu
from jax.sharding import PartitionSpec as P

NORM_EPS = 1e-5
F32 = jnp.float32
BF16 = jnp.bfloat16
MESH = pl.DeviceIdType.MESH
ANY = pl.BlockSpec(memory_space=pl.ANY)
VMEM = pl.BlockSpec(memory_space=pltpu.VMEM)
AG_COPIES = 11
RS_COPIES = 10
NN = (((1,), (0,)), ((), ()))
NT = (((1,), (1,)), ((), ()))
TN = (((0,), (0,)), ((), ()))


def dot(a, b, dims=NN):
    return lax.dot_general(a, b, dims, preferred_element_type=F32)


def aligned(index, size):
    return pl.ds(pl.multiple_of(index * size, size), size)


class Ring:
    def __init__(self, devices, rows, send_sems, recv_sems):
        self.chips = devices // 2
        self.rows = rows
        self.send_sems, self.recv_sems = send_sems, recv_sems
        self.used = 0
        self.me = lax.axis_index('tp')
        self.chip = self.me // 2
        self.core = self.me % 2
        self.right_chip = lax.rem(self.chip + 1, self.chips)
        self.left_chip = lax.rem(self.chip + self.chips - 1, self.chips)
        self.far_chip = lax.rem(self.chip + 2, self.chips)
        self.right = self.right_chip * 2 + self.core
        self.left = self.left_chip * 2 + self.core
        self.far = self.far_chip * 2 + self.core
        self.partner = self.chip * 2 + 1 - self.core
        self.peers = (self.left, self.right, self.partner)

    def greet(self):
        barrier = pltpu.get_barrier_semaphore()
        for peer in self.peers:
            pl.semaphore_signal(barrier, inc=1, device_id={'tp': peer}, device_id_type=MESH)
        pl.semaphore_wait(barrier, len(self.peers))

    def send(self, src, dst, device):
        copy = pltpu.make_async_remote_copy(src, dst, self.send_sems.at[self.used], self.recv_sems.at[self.used],
                                            device_id={'tp': device}, device_id_type=MESH)
        self.used += 1
        copy.start()
        return copy


class Gather:
    def __init__(self, ring, full):
        self.ring, self.full = ring, full
        self.half = ring.rows // 2

    def block(self, owner):
        return self.full.at[aligned(owner, self.ring.rows)]

    def part(self, owner, index):
        return self.full.at[pl.ds(pl.multiple_of(owner * self.ring.rows + index * self.half, self.half), self.half)]

    def start(self):
        ring = self.ring
        low, high, whole = self.part(ring.me, 0), self.part(ring.me, 1), self.block(ring.me)
        self.r0 = ring.send(low, low, ring.right)
        self.l1 = ring.send(high, high, ring.left)
        self.r1 = ring.send(high, high, ring.right)
        self.l0 = ring.send(low, low, ring.left)
        self.own = ring.send(whole, whole, ring.partner)

    def relay(self):
        ring = self.ring
        from_left, from_right = self.part(ring.left, 0), self.part(ring.right, 1)
        self.r0.wait_recv()
        self.relay_r = ring.send(from_left, from_left, ring.right)
        self.l1.wait_recv()
        self.relay_l = ring.send(from_right, from_right, ring.left)
        self.r1.wait_recv()
        left_block = self.block(ring.left)
        self.pass_left = ring.send(left_block, left_block, ring.partner)
        self.l0.wait_recv()
        right_block = self.block(ring.right)
        self.pass_right = ring.send(right_block, right_block, ring.partner)

    def finish(self):
        ring = self.ring
        far_low, far_high = self.part(ring.far, 0), self.part(ring.far, 1)
        self.relay_r.wait_recv()
        self.pass_low = ring.send(far_low, far_low, ring.partner)
        self.relay_l.wait_recv()
        self.pass_high = ring.send(far_high, far_high, ring.partner)
        for copy in (self.own, self.pass_left, self.pass_right, self.pass_low, self.pass_high):
            copy.wait_recv()

    def sent(self):
        for copy in (self.r0, self.l1, self.r1, self.l0, self.own, self.relay_r, self.relay_l, self.pass_left,
                     self.pass_right, self.pass_low, self.pass_high):
            copy.wait_send()


class Reduce:
    def __init__(self, ring, part, bufs):
        self.ring, self.part = ring, part
        self.from_partner, self.sums, self.via_left, self.via_right, self.in_left, self.in_right = bufs
        self.half = ring.rows // 2
        self.chips = (ring.far_chip, ring.right_chip, ring.left_chip, ring.chip)

    def start(self):
        ring = self.ring
        self.swaps = []
        for slot, chip in enumerate(self.chips):
            rows = self.part.at[aligned(chip * 2 + 1 - ring.core, ring.rows)]
            self.swaps.append(ring.send(rows, self.from_partner.at[slot], ring.partner))

    def add(self, slot):
        self.swaps[slot].wait_recv()
        rows = aligned(self.chips[slot] * 2 + self.ring.core, self.ring.rows)
        self.sums[slot] = self.part[rows, :] + self.from_partner[slot]

    def far_out(self):
        ring, half = self.ring, self.half
        self.add(0)
        self.far_r = ring.send(self.sums.at[0, 0:half], self.via_left, ring.right)
        self.far_l = ring.send(self.sums.at[0, half:2 * half], self.via_right, ring.left)

    def near_out(self):
        ring, half = self.ring, self.half
        self.add(1)
        self.near_r = ring.send(self.sums.at[1, half:2 * half], self.in_left.at[half:2 * half], ring.right)
        self.add(2)
        self.near_l = ring.send(self.sums.at[2, 0:half], self.in_right.at[0:half], ring.left)
        self.add(3)

    def relay(self):
        ring, half = self.ring, self.half
        self.far_r.wait_recv()
        self.sums[1, 0:half] = self.sums[1, 0:half] + self.via_left[...]
        self.relay_r = ring.send(self.sums.at[1, 0:half], self.in_left.at[0:half], ring.right)
        self.far_l.wait_recv()
        self.sums[2, half:2 * half] = self.sums[2, half:2 * half] + self.via_right[...]
        self.relay_l = ring.send(self.sums.at[2, half:2 * half], self.in_right.at[half:2 * half], ring.left)

    def finish(self):
        for copy in (self.near_r, self.near_l, self.relay_r, self.relay_l):
            copy.wait_recv()
        return self.sums[3] + self.in_left[...] + self.in_right[...]

    def sent(self):
        for copy in (*self.swaps, self.far_r, self.far_l, self.near_r, self.near_l, self.relay_r, self.relay_l):
            copy.wait_send()


def reduce_scratch(rows, width):
    return [pltpu.VMEM((4, rows, width), F32), pltpu.VMEM((4, rows, width), F32),
            pltpu.VMEM((rows // 2, width), F32), pltpu.VMEM((rows // 2, width), F32),
            pltpu.VMEM((rows, width), F32), pltpu.VMEM((rows, width), F32)]


REDUCE_BUFS = 6


def norm_rows(row_vals, gain_vec):
    vals = row_vals.astype(F32)
    return (vals * lax.rsqrt(jnp.mean(vals * vals, axis=-1, keepdims=True) + NORM_EPS) * gain_vec).astype(BF16)


def norm_rows_backward(row_vals, gain_vec, cot_rows):
    vals = row_vals.astype(F32)
    scale = lax.rsqrt(jnp.mean(vals * vals, axis=-1, keepdims=True) + NORM_EPS)
    unit = vals * scale
    grad_gain = jnp.sum(cot_rows * unit, axis=0, keepdims=True)
    cot_unit = cot_rows * gain_vec
    grad_vals = scale * (cot_unit - unit * jnp.mean(cot_unit * unit, axis=-1, keepdims=True))
    return grad_vals, grad_gain


def head_probs(query, key, score_scale):
    seq_len = query.shape[0]
    scores = dot(query, key, NT) * score_scale
    row_pos = lax.broadcasted_iota(jnp.int32, (seq_len, seq_len), 0)
    col_pos = lax.broadcasted_iota(jnp.int32, (seq_len, seq_len), 1)
    scores = jnp.where(row_pos >= col_pos, scores, -1e30)
    exp_scores = jnp.exp(scores - jnp.max(scores, axis=-1, keepdims=True))
    return exp_scores / jnp.sum(exp_scores, axis=-1, keepdims=True)


def residual(row_vals, total):
    return (row_vals.astype(F32) + total.astype(BF16).astype(F32)).astype(BF16)


def loop(count, body):
    def step(index, carry):
        body(index)
        return carry
    lax.fori_loop(0, count, step, 0)


class AttentionBlock:
    def __init__(self, env, layer):
        self.env, self.layer = env, layer
        self.weights = ((env.w_qkv, env.qkv_w, env.grad_qkv_out), (env.w_out, env.out_w, env.grad_out_out))
        self.sems = (0, 1)
        self.rows_ref = env.layer_rows.at[layer]
        self.gain = env.gain_attn[layer:layer + 1, :]
        self.gain_row = layer
        self.scale = env.head_dim ** -0.5
        self.qkv = env.qkv.at[layer]
        self.mix = env.mix.at[layer]

    def cols(self, slot):
        return slice(slot * self.env.head_dim, (slot + 1) * self.env.head_dim)

    def gathered(self, micro):
        self.qkv[micro] = dot(self.env.full[...], self.env.qkv_w[...]).astype(BF16)

    def forward(self, micro):
        env = self.env
        key = self.qkv[micro, :, self.cols(env.groups)]
        value = self.qkv[micro, :, self.cols(env.groups + 1)]
        for head in range(env.groups):
            cols = self.cols(head)
            prob = head_probs(self.qkv[micro, :, cols], key, self.scale).astype(BF16)
            self.mix[micro, :, cols] = dot(prob, value).astype(BF16)

        def columns(index):
            cols = aligned(index, 512)
            env.part[micro, :, cols] = dot(self.mix[micro], env.out_w[:, cols])
        loop(env.out_w.shape[1] // 512, columns)

    def backward(self, micro, cot):
        env = self.env
        groups = env.groups
        env.grad_mix[...] = dot(cot[...], env.out_w[...], NT).astype(BF16)
        key = self.qkv[micro, :, self.cols(groups)]
        value = self.qkv[micro, :, self.cols(groups + 1)]
        grad_key = grad_value = None
        for head in range(groups):
            cols = self.cols(head)
            query = self.qkv[micro, :, cols]
            head_grad = env.grad_mix[:, cols]
            prob = head_probs(query, key, self.scale)
            grad_prob = dot(head_grad, value, NT).astype(BF16).astype(F32)
            row_dot = jnp.sum(grad_prob * prob, axis=-1, keepdims=True)
            grad_scores = (prob * (grad_prob - row_dot) * self.scale).astype(BF16)
            env.grad_qkv[:, cols] = dot(grad_scores, key).astype(BF16)
            key_term = dot(grad_scores, query, TN)
            value_term = dot(prob.astype(BF16), head_grad, TN)
            grad_key = key_term if grad_key is None else grad_key + key_term
            grad_value = value_term if grad_value is None else grad_value + value_term
        env.grad_qkv[:, self.cols(groups)] = grad_key.astype(BF16)
        env.grad_qkv[:, self.cols(groups + 1)] = grad_value.astype(BF16)

        def columns(index):
            cols = aligned(index, 256)
            env.part[micro, :, cols] = dot(env.grad_qkv[...], env.qkv_w[cols, :], NT)
        loop(env.qkv_w.shape[0] // 256, columns)

    def weights_near(self, micro):
        env = self.env

        def columns(index):
            cols = aligned(index, 256)
            env.put(micro, env.acc_qkv, env.qkv_w, cols, dot(env.full[:, cols], env.grad_qkv[...], TN))
        loop(env.full.shape[1] // 256, columns)
        return (0,) if micro else ()

    def weights_far(self, cots):
        env = self.env

        def columns(index):
            cols = aligned(index, 128)
            env.out_w[cols, :] = (dot(self.mix[0, :, cols], cots[0][...], TN)
                                  + dot(self.mix[1, :, cols], cots[1][...], TN)).astype(BF16)
        loop(env.out_w.shape[0] // 128, columns)
        return (1,)


class MlpBlock:
    def __init__(self, env, layer):
        self.env, self.layer = env, layer
        self.weights = ((env.w_gate, env.gate_w, env.grad_gate_out), (env.w_up, env.up_w, env.grad_up_out),
                        (env.w_down, env.down_w, env.grad_down_out))
        self.sems = (2, 3, 4)
        self.rows_ref = env.hidden_rows.at[layer]
        self.gain = env.gain_mlp[layer:layer + 1, :]
        self.gain_row = env.layers + layer

    def gathered(self, micro):
        env = self.env

        def columns(index):
            cols = aligned(index, 256)
            gate_pre = dot(env.full[...], env.gate_w[:, cols])
            up_proj = dot(env.full[...], env.up_w[:, cols])
            env.inner[micro, :, cols] = (gate_pre * jax.nn.sigmoid(gate_pre) * up_proj).astype(BF16)
        loop(env.gate_w.shape[1] // 256, columns)

    def forward(self, micro):
        env = self.env

        def columns(index):
            cols = aligned(index, 512)
            env.part[micro, :, cols] = dot(env.inner[micro], env.down_w[:, cols])
        loop(env.down_w.shape[1] // 512, columns)

    def backward(self, micro, cot):
        env = self.env

        def columns(index):
            cols = aligned(index, 256)
            gate_pre = dot(env.full[...], env.gate_w[:, cols])
            up_proj = dot(env.full[...], env.up_w[:, cols])
            grad_inner = dot(cot[...], env.down_w[cols, :], NT).astype(BF16).astype(F32)
            gate_sig = jax.nn.sigmoid(gate_pre)
            gate_act = gate_pre * gate_sig
            env.inner[micro, :, cols] = (gate_act * up_proj).astype(BF16)
            env.grad_up[:, cols] = (grad_inner * gate_act).astype(BF16)
            env.grad_gate[:, cols] = (grad_inner * up_proj * gate_sig * (1.0 + gate_pre * (1.0 - gate_sig))).astype(BF16)
        loop(env.gate_w.shape[1] // 256, columns)

        def out_columns(index):
            cols = aligned(index, 256)
            env.part[micro, :, cols] = (dot(env.grad_gate[...], env.gate_w[cols, :], NT)
                                        + dot(env.grad_up[...], env.up_w[cols, :], NT))
        loop(env.gate_w.shape[0] // 256, out_columns)

    def weights_near(self, micro):
        env = self.env

        def columns(index):
            cols = aligned(index, 256)
            env.put(micro, env.acc_gate, env.gate_w, cols, dot(env.full[:, cols], env.grad_gate[...], TN))
            env.put(micro, env.acc_up, env.up_w, cols, dot(env.full[:, cols], env.grad_up[...], TN))
        loop(env.full.shape[1] // 256, columns)
        return (0, 1) if micro else ()

    def weights_far(self, cots):
        env = self.env

        def columns(index):
            cols = aligned(index, 128)
            env.down_w[cols, :] = (dot(env.inner[0, :, cols], cots[0][...], TN)
                                   + dot(env.inner[1, :, cols], cots[1][...], TN)).astype(BF16)
        loop(env.down_w.shape[0] // 128, columns)
        return (2,)


FORWARD_ORDER = 'XEfrnR'
BACKWARD_ORDER = 'EXrfwVnRvW'


class Env:
    def __init__(self, names, refs, **sizes):
        self.__dict__.update(zip(names, refs))
        self.__dict__.update(sizes)

    def put(self, micro, acc, stage, rows, term):
        if micro == 0:
            acc[rows, :] = term
        else:
            stage[rows, :] = (acc[rows, :] + term).astype(BF16)


def stack_kernel(names, sizes, *refs):
    env = Env(names, refs, **sizes)
    layers, devices = env.layers, env.devices
    ring = Ring(devices, env.x_in.shape[1], env.send_sems, env.recv_sems)
    own = aligned(ring.me, ring.rows)
    blocks = []
    for layer in range(layers):
        blocks += [AttentionBlock(env, layer), MlpBlock(env, layer)]

    def load(block):
        copies = [pltpu.make_async_copy(src.at[block.layer], dst, env.load_sems.at[sem])
                  for (src, dst, unused), sem in zip(block.weights, block.sems)]
        for copy in copies:
            copy.start()
        return copies

    stores = {}
    loads = {block: load(block) for block in blocks[:2]}

    def need(block):
        for copy in loads.pop(block, ()):
            copy.wait()

    def store(block, indices):
        for index in indices:
            unused, src, dst = block.weights[index]
            copy = pltpu.make_async_copy(src, dst.at[block.layer], env.store_sems.at[block.sems[index]])
            copy.start()
            stores.setdefault(block, []).append(copy)

    barrier = pltpu.get_barrier_semaphore()
    others = [lax.rem(ring.me + step, devices) for step in range(1, devices)]
    for peer in others:
        pl.semaphore_signal(barrier, inc=1, device_id={'tp': peer}, device_id_type=MESH)
    pl.semaphore_wait(barrier, len(others))

    uses = []

    def full_start(block, micro):
        if uses:
            pl.semaphore_wait(env.credit, len(ring.peers))
        uses.append(block)
        env.full[own, :] = norm_rows(block.rows_ref[micro], block.gain)
        ring.used = 0
        gather = Gather(ring, env.full)
        gather.start()
        ring.used = AG_COPIES
        return gather

    def resume(index):
        ring.used = index

    total_uses = 2 * len(blocks) * 2

    def full_done(gather):
        gather.sent()
        if len(uses) < total_uses:
            for peer in ring.peers:
                pl.semaphore_signal(env.credit, inc=1, device_id={'tp': peer}, device_id_type=MESH)

    def gather_base(micro):
        return AG_COPIES * (1 + micro)

    def reduce_base(micro):
        return AG_COPIES * 3 + RS_COPIES * micro

    def staged(base, start, step):
        resume(base + start)
        return step()

    def relay(gather, base):
        staged(base, 5, gather.relay)

    def finish(gather, base):
        staged(base, 9, gather.finish)

    reducers = [None, None]

    def reduce_start(micro):
        reducer = Reduce(ring, env.part.at[micro], tuple(buf.at[micro] for buf in (
            env.from_partner, env.sums, env.via_left, env.via_right, env.in_left, env.in_right)))
        reducers[micro] = reducer
        staged(reduce_base(micro), 0, reducer.start)

    def reduce_far(micro):
        staged(reduce_base(micro), 4, reducers[micro].far_out)

    def reduce_near(micro):
        staged(reduce_base(micro), 6, reducers[micro].near_out)

    def reduce_relay(micro):
        staged(reduce_base(micro), 8, reducers[micro].relay)

    def reduce_finish(micro):
        total = reducers[micro].finish()
        reducers[micro].sent()
        reducers[micro] = None
        return total

    def after_forward(index, micro):
        total = reduce_finish(micro)
        block = blocks[index]
        rows = residual(block.rows_ref[micro], total)
        if index + 1 < len(blocks):
            blocks[index + 1].rows_ref[micro] = rows
        else:
            env.y_out[micro] = rows

    for micro in range(2):
        blocks[0].rows_ref[micro] = env.x_in[micro]
    back = blocks[::-1]
    cot_rows = env.cot_rows
    for micro in range(2):
        cot_rows[0, micro] = env.y_cot[micro]
    cot_gathers = [None, None]

    def cot_start(index, micro):
        cots = env.cots.at[index % 2, micro]
        cots[own, :] = cot_rows[index % 2, micro]
        resume(gather_base(micro))
        cot_gathers[micro] = Gather(ring, cots)
        cot_gathers[micro].start()

    gather = full_start(blocks[0], 0)
    relay(gather, 0)
    for index, block in enumerate(blocks):
        last = index + 1 == len(blocks)
        for micro in range(2):
            finish(gather, 0)
            need(block)
            block.gathered(micro)
            full_done(gather)
            for step in FORWARD_ORDER:
                if step == 'X':
                    block.forward(micro)
                    reduce_start(micro)
                elif step == 'E':
                    if micro == 0:
                        if index > 0:
                            after_forward(index - 1, 1)
                        gather = full_start(block, 1)
                    else:
                        after_forward(index, 0)
                        if last:
                            cot_start(0, 0)
                        gather = full_start(back[0] if last else blocks[index + 1], 0)
                elif step == 'f':
                    reduce_far(micro)
                elif step == 'r':
                    if last and micro == 1:
                        relay(cot_gathers[0], gather_base(0))
                    relay(gather, 0)
                elif step == 'n':
                    reduce_near(micro)
                else:
                    reduce_relay(micro)
        if index + 2 < len(blocks):
            loads[blocks[index + 2]] = load(blocks[index + 2])

    def after_backward(index, micro):
        total = reduce_finish(micro).astype(BF16).astype(F32)
        block = back[index]
        grad_rows, grad_gain = norm_rows_backward(block.rows_ref[micro], block.gain, total)
        rows = (cot_rows[index % 2, micro].astype(F32) + grad_rows).astype(BF16)
        gain_row = slice(block.gain_row, block.gain_row + 1)
        env.gains[gain_row, :] = grad_gain if micro == 0 else env.gains[gain_row, :] + grad_gain
        if index + 1 < len(back):
            cot_rows[(index + 1) % 2, micro] = rows
        else:
            env.grad_x[micro] = rows

    for index, block in enumerate(back):
        last = index + 1 == len(back)
        for micro in range(2):
            other = 1 - micro
            finish(cot_gathers[micro], gather_base(micro))
            finish(gather, 0)
            need(block)
            going = micro == 0 or not last
            for step in BACKWARD_ORDER:
                if step == 'X':
                    block.backward(micro, env.cots.at[index % 2, micro])
                    reduce_start(micro)
                elif step == 'E':
                    if micro == 1:
                        after_backward(index, 0)
                    elif index == 0:
                        after_forward(len(blocks) - 1, 1)
                    else:
                        after_backward(index - 1, 1)
                    if going:
                        cot_start(index + micro, other)
                elif step == 'f':
                    reduce_far(micro)
                elif step == 'w':
                    store(block, block.weights_near(micro))
                    full_done(gather)
                    cot_gathers[micro].sent()
                elif step == 'r':
                    if going:
                        relay(cot_gathers[other], gather_base(other))
                elif step == 'V':
                    if going:
                        gather = full_start(block if micro == 0 else back[index + 1], other)
                elif step == 'n':
                    reduce_near(micro)
                elif step == 'R':
                    reduce_relay(micro)
                elif step == 'v':
                    if going:
                        relay(gather, 0)
                elif micro == 1:
                    store(block, block.weights_far([env.cots.at[index % 2, 0], env.cots.at[index % 2, 1]]))
                elif index > 0 and not last:
                    for copy in stores.pop(back[index - 1], ()):
                        copy.wait()
                    loads[back[index + 1]] = load(back[index + 1])
    after_backward(len(back) - 1, 1)

    copies = []
    for index, peer in enumerate(others):
        copy = pltpu.make_async_remote_copy(env.gains, env.gain_parts.at[ring.me], env.gain_send.at[index],
                                            env.gain_recv.at[index], device_id={'tp': peer}, device_id_type=MESH)
        copy.start()
        copies.append(copy)
    env.gain_parts[ring.me] = env.gains[...]
    for copy in copies:
        copy.wait()
    total = env.gain_parts[0]
    for index in range(1, devices):
        total = total + env.gain_parts[index]
    env.gain_out[...] = total
    for copies in stores.values():
        for copy in copies:
            copy.wait()


def comm_params(collective_id):
    return pltpu.CompilerParams(collective_id=collective_id, has_side_effects=True, vmem_limit_bytes=66_000_000)


def solution(mesh):
    devices = mesh.shape['tp']
    row_spec = P(None, ('dp', 'tp'), None)
    gain_spec = P(None, None)
    qkv_spec = P(None, None, 'tp', None, None)
    head_spec = P(None, 'tp', None, None)
    col_spec = P(None, None, 'tp')
    row_shard_spec = P(None, 'tp', None)

    def device_program(x_in, y_cot, gain_attn, gain_mlp, w_qkv, w_out, w_gate, w_up, w_down):
        micros, rows, width = x_in.shape
        layers = w_qkv.shape[0]
        groups = w_qkv.shape[3] - 2
        head_dim = w_qkv.shape[4]
        seq_len = rows * devices
        qkv_width = (groups + 2) * head_dim
        mix_width = groups * head_dim
        inner_width = w_gate.shape[2]
        inputs = {
            'x_in': (x_in, VMEM), 'y_cot': (y_cot, VMEM), 'gain_attn': (gain_attn, VMEM), 'gain_mlp': (gain_mlp, VMEM),
            'w_qkv': (w_qkv.reshape(layers, width, qkv_width), ANY), 'w_out': (w_out.reshape(layers, mix_width, width), ANY),
            'w_gate': (w_gate, ANY), 'w_up': (w_up, ANY), 'w_down': (w_down, ANY)}

        def out(shape, dtype, spec):
            return jax.ShapeDtypeStruct(shape, dtype), spec

        outputs = {
            'y_out': out(x_in.shape, BF16, VMEM), 'grad_x': out(x_in.shape, BF16, VMEM),
            'grad_qkv_out': out((layers, width, qkv_width), BF16, ANY), 'grad_out_out': out((layers, mix_width, width), BF16, ANY),
            'grad_gate_out': out(w_gate.shape, BF16, ANY), 'grad_up_out': out(w_up.shape, BF16, ANY),
            'grad_down_out': out(w_down.shape, BF16, ANY), 'gain_out': out((2 * layers, width), F32, VMEM)}

        def bf16(*shape):
            return pltpu.VMEM(shape, BF16)

        def f32(*shape):
            return pltpu.VMEM(shape, F32)

        def dma(count):
            return pltpu.SemaphoreType.DMA((count,))

        copies = 3 * AG_COPIES + 2 * RS_COPIES
        scratch = {
            'layer_rows': bf16(layers, micros, rows, width), 'hidden_rows': bf16(layers, micros, rows, width),
            'cot_rows': bf16(2, micros, rows, width), 'qkv': bf16(layers, micros, seq_len, qkv_width),
            'mix': bf16(layers, micros, seq_len, mix_width), 'inner': bf16(micros, seq_len, inner_width),
            'grad_gate': bf16(seq_len, inner_width), 'grad_up': bf16(seq_len, inner_width),
            'grad_mix': bf16(seq_len, mix_width), 'grad_qkv': bf16(seq_len, qkv_width),
            'qkv_w': bf16(width, qkv_width), 'out_w': bf16(mix_width, width), 'gate_w': bf16(width, inner_width),
            'up_w': bf16(width, inner_width), 'down_w': bf16(inner_width, width),
            'acc_qkv': f32(width, qkv_width), 'acc_gate': f32(width, inner_width), 'acc_up': f32(width, inner_width),
            'full': bf16(seq_len, width), 'cots': bf16(2, micros, seq_len, width), 'part': f32(micros, seq_len, width),
            'from_partner': f32(micros, 4, rows, width), 'sums': f32(micros, 4, rows, width),
            'via_left': f32(micros, rows // 2, width), 'via_right': f32(micros, rows // 2, width),
            'in_left': f32(micros, rows, width), 'in_right': f32(micros, rows, width),
            'gains': f32(2 * layers, width), 'gain_parts': f32(devices, 2 * layers, width),
            'load_sems': dma(5), 'store_sems': dma(5), 'send_sems': dma(copies), 'recv_sems': dma(copies),
            'gain_send': dma(devices - 1), 'gain_recv': dma(devices - 1), 'credit': pltpu.SemaphoreType.REGULAR}
        names = (*inputs, *outputs, *scratch)
        sizes = dict(layers=layers, devices=devices, groups=groups, head_dim=head_dim)
        results = pl.pallas_call(
            functools.partial(stack_kernel, names, sizes),
            out_shape=tuple(shape for shape, spec in outputs.values()),
            in_specs=[spec for array, spec in inputs.values()], out_specs=tuple(spec for shape, spec in outputs.values()),
            scratch_shapes=list(scratch.values()), compiler_params=comm_params(0), name='stack',
        )(*(array for array, spec in inputs.values()))
        y_rows, grad_rows, grad_qkv, grad_out, grad_gate, grad_up, grad_down, gain_sum = results
        return (y_rows, grad_rows, grad_qkv.reshape(w_qkv.shape), grad_out.reshape(w_out.shape), grad_gate, grad_up, grad_down,
                gain_sum[:layers], gain_sum[layers:])

    return jax.shard_map(device_program, mesh=mesh,
                         in_specs=(row_spec, row_spec, gain_spec, gain_spec, qkv_spec, head_spec, col_spec, col_spec, row_shard_spec),
                         out_specs=(row_spec, row_spec, P('dp', None, 'tp', None, None), P('dp', 'tp', None, None), P('dp', None, 'tp'), P('dp', None, 'tp'), P('dp', 'tp', None), P('dp', None), P('dp', None)),
                         check_vma=False)
```

```python
import functools

import jax
import jax.numpy as jnp
from jax import lax
from jax.experimental import pallas as pl
from jax.experimental.pallas import tpu as pltpu
from jax.sharding import PartitionSpec as P

NORM_EPS = 1e-5
F32 = jnp.float32
BF16 = jnp.bfloat16
MESH = pl.DeviceIdType.MESH
ANY = pl.BlockSpec(memory_space=pl.ANY)
VMEM = pl.BlockSpec(memory_space=pltpu.VMEM)
AG_COPIES = 11
RS_COPIES = 10
HALVES = 1
NN = (((1,), (0,)), ((), ()))
NT = (((1,), (1,)), ((), ()))
TN = (((0,), (0,)), ((), ()))


def dot(a, b, dims=NN):
    return lax.dot_general(a, b, dims, preferred_element_type=F32)


def aligned(index, size):
    return pl.ds(pl.multiple_of(index * size, size), size)


class Ring:
    def __init__(self, devices, rows, send_sems, recv_sems):
        self.chips = devices // 2
        self.rows = rows
        self.send_sems, self.recv_sems = send_sems, recv_sems
        self.used = 0
        self.me = lax.axis_index('tp')
        self.chip = self.me // 2
        self.core = self.me % 2
        self.right_chip = lax.rem(self.chip + 1, self.chips)
        self.left_chip = lax.rem(self.chip + self.chips - 1, self.chips)
        self.far_chip = lax.rem(self.chip + 2, self.chips)
        self.right = self.right_chip * 2 + self.core
        self.left = self.left_chip * 2 + self.core
        self.far = self.far_chip * 2 + self.core
        self.partner = self.chip * 2 + 1 - self.core
        self.peers = (self.left, self.right, self.partner)

    def greet(self):
        barrier = pltpu.get_barrier_semaphore()
        for peer in self.peers:
            pl.semaphore_signal(barrier, inc=1, device_id={'tp': peer}, device_id_type=MESH)
        pl.semaphore_wait(barrier, len(self.peers))

    def send(self, src, dst, device):
        copy = pltpu.make_async_remote_copy(src, dst, self.send_sems.at[self.used], self.recv_sems.at[self.used],
                                            device_id={'tp': device}, device_id_type=MESH)
        self.used += 1
        copy.start()
        return copy


class Gather:
    def __init__(self, ring, full):
        self.ring, self.full = ring, full
        self.half = ring.rows // 2

    def block(self, owner):
        return self.full.at[aligned(owner, self.ring.rows)]

    def part(self, owner, index):
        return self.full.at[pl.ds(pl.multiple_of(owner * self.ring.rows + index * self.half, self.half), self.half)]

    def start(self):
        ring = self.ring
        low, high, whole = self.part(ring.me, 0), self.part(ring.me, 1), self.block(ring.me)
        self.r0 = ring.send(low, low, ring.right)
        self.l1 = ring.send(high, high, ring.left)
        self.r1 = ring.send(high, high, ring.right)
        self.l0 = ring.send(low, low, ring.left)
        self.own = ring.send(whole, whole, ring.partner)

    def relay(self):
        ring = self.ring
        from_left, from_right = self.part(ring.left, 0), self.part(ring.right, 1)
        self.r0.wait_recv()
        self.relay_r = ring.send(from_left, from_left, ring.right)
        self.l1.wait_recv()
        self.relay_l = ring.send(from_right, from_right, ring.left)
        self.r1.wait_recv()
        left_block = self.block(ring.left)
        self.pass_left = ring.send(left_block, left_block, ring.partner)
        self.l0.wait_recv()
        right_block = self.block(ring.right)
        self.pass_right = ring.send(right_block, right_block, ring.partner)

    def finish(self):
        ring = self.ring
        far_low, far_high = self.part(ring.far, 0), self.part(ring.far, 1)
        self.relay_r.wait_recv()
        self.pass_low = ring.send(far_low, far_low, ring.partner)
        self.relay_l.wait_recv()
        self.pass_high = ring.send(far_high, far_high, ring.partner)
        for copy in (self.own, self.pass_left, self.pass_right, self.pass_low, self.pass_high):
            copy.wait_recv()

    def sent(self):
        for copy in (self.r0, self.l1, self.r1, self.l0, self.own, self.relay_r, self.relay_l, self.pass_left,
                     self.pass_right, self.pass_low, self.pass_high):
            copy.wait_send()


class Reduce:
    def __init__(self, ring, part, bufs):
        self.ring, self.part = ring, part
        self.from_partner, self.sums, self.via_left, self.via_right, self.in_left, self.in_right = bufs
        self.half = ring.rows // 2
        self.chips = (ring.far_chip, ring.right_chip, ring.left_chip, ring.chip)

    def start(self):
        ring = self.ring
        self.swaps = []
        for slot, chip in enumerate(self.chips):
            rows = self.part.at[aligned(chip * 2 + 1 - ring.core, ring.rows)]
            self.swaps.append(ring.send(rows, self.from_partner.at[slot], ring.partner))

    def add(self, slot):
        self.swaps[slot].wait_recv()
        rows = aligned(self.chips[slot] * 2 + self.ring.core, self.ring.rows)
        self.sums[slot] = self.part[rows, :] + self.from_partner[slot]

    def far_out(self):
        ring, half = self.ring, self.half
        self.add(0)
        self.far_r = ring.send(self.sums.at[0, 0:half], self.via_left, ring.right)
        self.far_l = ring.send(self.sums.at[0, half:2 * half], self.via_right, ring.left)

    def near_out(self):
        ring, half = self.ring, self.half
        self.add(1)
        self.near_r = ring.send(self.sums.at[1, half:2 * half], self.in_left.at[half:2 * half], ring.right)
        self.add(2)
        self.near_l = ring.send(self.sums.at[2, 0:half], self.in_right.at[0:half], ring.left)
        self.add(3)

    def relay(self):
        ring, half = self.ring, self.half
        self.far_r.wait_recv()
        self.sums[1, 0:half] = self.sums[1, 0:half] + self.via_left[...]
        self.relay_r = ring.send(self.sums.at[1, 0:half], self.in_left.at[0:half], ring.right)
        self.far_l.wait_recv()
        self.sums[2, half:2 * half] = self.sums[2, half:2 * half] + self.via_right[...]
        self.relay_l = ring.send(self.sums.at[2, half:2 * half], self.in_right.at[half:2 * half], ring.left)

    def finish(self):
        for copy in (self.near_r, self.near_l, self.relay_r, self.relay_l):
            copy.wait_recv()
        return self.sums[3] + self.in_left[...] + self.in_right[...]

    def sent(self):
        for copy in (*self.swaps, self.far_r, self.far_l, self.near_r, self.near_l, self.relay_r, self.relay_l):
            copy.wait_send()


def reduce_scratch(rows, width):
    return [pltpu.VMEM((4, rows, width), F32), pltpu.VMEM((4, rows, width), F32),
            pltpu.VMEM((rows // 2, width), F32), pltpu.VMEM((rows // 2, width), F32),
            pltpu.VMEM((rows, width), F32), pltpu.VMEM((rows, width), F32)]


REDUCE_BUFS = 6


def norm_rows(row_vals, gain_vec):
    vals = row_vals.astype(F32)
    return (vals * lax.rsqrt(jnp.mean(vals * vals, axis=-1, keepdims=True) + NORM_EPS) * gain_vec).astype(BF16)


def norm_unit(row_vals):
    vals = row_vals.astype(F32)
    scale = lax.rsqrt(jnp.mean(vals * vals, axis=-1, keepdims=True) + NORM_EPS)
    return vals * scale, scale


def norm_rows_backward(unit, scale, gain_vec, cot_rows):
    cot_unit = cot_rows * gain_vec
    return scale * (cot_unit - unit * jnp.mean(cot_unit * unit, axis=-1, keepdims=True))


def head_probs(query, key, score_scale):
    seq_len = query.shape[0]
    scores = dot(query, key, NT) * score_scale
    row_pos = lax.broadcasted_iota(jnp.int32, (seq_len, seq_len), 0)
    col_pos = lax.broadcasted_iota(jnp.int32, (seq_len, seq_len), 1)
    scores = jnp.where(row_pos >= col_pos, scores, -1e30)
    exp_scores = jnp.exp(scores - jnp.max(scores, axis=-1, keepdims=True))
    return exp_scores / jnp.sum(exp_scores, axis=-1, keepdims=True)


def residual(row_vals, total):
    return (row_vals.astype(F32) + total.astype(BF16).astype(F32)).astype(BF16)


def loop(count, body):
    def step(index, carry):
        body(index)
        return carry
    lax.fori_loop(0, count, step, 0)


class AttentionBlock:
    def __init__(self, env, layer):
        self.env, self.layer = env, layer
        self.weights = ((env.stage_qkv, env.grad_qkv_out), (env.out_w, env.grad_out_out))
        self.loads = [(env.w_qkv.at[layer], env.qkv_w), (env.w_out.at[layer], env.out_w)]
        self.load_base = 3
        self.sems = (0, 1)
        self.rows_ref = env.layer_rows.at[layer]
        self.gain = env.gain_attn[layer:layer + 1, :]
        self.gain_row = layer
        self.scale = env.head_dim ** -0.5
        self.qkv = env.qkv.at[layer]
        self.mix = env.mix.at[layer]

    def cols(self, slot):
        return slice(slot * self.env.head_dim, (slot + 1) * self.env.head_dim)

    def gathered(self, micro):
        self.qkv[micro] = dot(self.env.full[...], self.env.qkv_w[...]).astype(BF16)

    def forward(self, micro):
        env = self.env
        key = self.qkv[micro, :, self.cols(env.groups)]
        value = self.qkv[micro, :, self.cols(env.groups + 1)]
        for head in range(env.groups):
            cols = self.cols(head)
            prob = head_probs(self.qkv[micro, :, cols], key, self.scale).astype(BF16)
            self.mix[micro, :, cols] = dot(prob, value).astype(BF16)

    def forward_partial(self, micro, half):
        env = self.env

        def columns(index):
            cols = aligned(index, 512)
            env.part[micro, half, :, cols] = dot(self.mix[micro], env.out_w[:, cols])
        loop(env.out_w.shape[1] // 512, columns)

    def backward(self, micro, cot):
        env = self.env
        groups = env.groups
        env.grad_mix[...] = dot(cot[...], env.out_w[...], NT).astype(BF16)
        key = self.qkv[micro, :, self.cols(groups)]
        value = self.qkv[micro, :, self.cols(groups + 1)]
        grad_key = grad_value = None
        for head in range(groups):
            cols = self.cols(head)
            query = self.qkv[micro, :, cols]
            head_grad = env.grad_mix[:, cols]
            prob = head_probs(query, key, self.scale)
            grad_prob = dot(head_grad, value, NT).astype(BF16).astype(F32)
            row_dot = jnp.sum(grad_prob * prob, axis=-1, keepdims=True)
            grad_scores = (prob * (grad_prob - row_dot) * self.scale).astype(BF16)
            env.grad_qkv[:, cols] = dot(grad_scores, key).astype(BF16)
            key_term = dot(grad_scores, query, TN)
            value_term = dot(prob.astype(BF16), head_grad, TN)
            grad_key = key_term if grad_key is None else grad_key + key_term
            grad_value = value_term if grad_value is None else grad_value + value_term
        env.grad_qkv[:, self.cols(groups)] = grad_key.astype(BF16)
        env.grad_qkv[:, self.cols(groups + 1)] = grad_value.astype(BF16)

    def backward_partial(self, micro, half):
        env = self.env

        def columns(index):
            cols = aligned(index, 256)
            env.part[micro, half, :, cols] = dot(env.grad_qkv[...], env.qkv_w[cols, :], NT)
        loop(env.qkv_w.shape[0] // 256, columns)

    def weights_near(self, second):
        env = self.env

        def columns(index):
            cols = aligned(index, 256)
            env.put(second, env.acc_qkv, env.stage_qkv, cols, dot(env.full[:, cols], env.grad_qkv[...], TN))
        loop(env.full.shape[1] // 256, columns)
        return (0,) if second else ()

    def weights_far(self, cots):
        env = self.env

        def columns(index):
            cols = aligned(index, 128)
            env.out_w[cols, :] = (dot(self.mix[0, :, cols], cots[0][...], TN)
                                  + dot(self.mix[1, :, cols], cots[1][...], TN)).astype(BF16)
        loop(env.out_w.shape[0] // 128, columns)
        return (1,)


class MlpBlock:
    def __init__(self, env, layer):
        self.env, self.layer = env, layer
        self.weights = ((env.stage_gate, env.grad_gate_out), (env.stage_up, env.grad_up_out), (env.down_w, env.grad_down_out))
        self.loads = [(env.w_gate.at[layer], env.gate_w), (env.w_up.at[layer], env.up_w), (env.w_down.at[layer], env.down_w)]
        self.load_base = 0
        self.sems = (2, 3, 4)
        self.rows_ref = env.hidden_rows.at[layer]
        self.gain = env.gain_mlp[layer:layer + 1, :]
        self.gain_row = env.layers + layer

    def gathered(self, micro):
        env = self.env

        def columns(index):
            cols = aligned(index, 256)
            gate_pre = dot(env.full[...], env.gate_w[:, cols])
            up_proj = dot(env.full[...], env.up_w[:, cols])
            env.inner[micro, :, cols] = (gate_pre * jax.nn.sigmoid(gate_pre) * up_proj).astype(BF16)
        loop(env.gate_w.shape[1] // 256, columns)

    def forward(self, micro):
        pass

    def forward_partial(self, micro, half):
        env = self.env

        def columns(index):
            cols = aligned(index, 512)
            env.part[micro, half, :, cols] = dot(env.inner[micro], env.down_w[:, cols])
        loop(env.down_w.shape[1] // 512, columns)

    def backward(self, micro, cot):
        env = self.env

        def columns(index):
            cols = aligned(index, 256)
            gate_pre = dot(env.full[...], env.gate_w[:, cols])
            up_proj = dot(env.full[...], env.up_w[:, cols])
            grad_inner = dot(cot[...], env.down_w[cols, :], NT).astype(BF16).astype(F32)
            gate_sig = jax.nn.sigmoid(gate_pre)
            gate_act = gate_pre * gate_sig
            env.inner[micro, :, cols] = (gate_act * up_proj).astype(BF16)
            env.grad_up[:, cols] = (grad_inner * gate_act).astype(BF16)
            env.grad_gate[:, cols] = (grad_inner * up_proj * gate_sig * (1.0 + gate_pre * (1.0 - gate_sig))).astype(BF16)
        loop(env.gate_w.shape[1] // 256, columns)

    def backward_partial(self, micro, half):
        env = self.env

        def columns(index):
            cols = aligned(index, 256)
            env.part[micro, half, :, cols] = (dot(env.grad_gate[...], env.gate_w[cols, :], NT)
                                              + dot(env.grad_up[...], env.up_w[cols, :], NT))
        loop(env.gate_w.shape[0] // 256, columns)

    def weights_near(self, second):
        env = self.env

        def columns(index):
            cols = aligned(index, 256)
            env.put(second, env.acc_gate, env.stage_gate, cols, dot(env.full[:, cols], env.grad_gate[...], TN))
            env.put(second, env.acc_up, env.stage_up, cols, dot(env.full[:, cols], env.grad_up[...], TN))
        loop(env.full.shape[1] // 256, columns)
        return (0, 1) if second else ()

    def weights_far(self, cots):
        env = self.env

        def columns(index):
            cols = aligned(index, 128)
            env.down_w[cols, :] = (dot(env.inner[0, :, cols], cots[0][...], TN)
                                   + dot(env.inner[1, :, cols], cots[1][...], TN)).astype(BF16)
        loop(env.down_w.shape[0] // 128, columns)
        return (2,)


FORWARD_ORDER = 'XEfrnR'
BACKWARD_ORDER = 'XwEVPfrvnRW'


class Env:
    def __init__(self, names, refs, **sizes):
        self.__dict__.update(zip(names, refs))
        self.__dict__.update(sizes)

    def put(self, second, acc, stage, rows, term):
        if second:
            stage[rows, :] = (acc[rows, :] + term).astype(BF16)
        else:
            acc[rows, :] = term


def stack_kernel(names, sizes, *refs):
    env = Env(names, refs, **sizes)
    layers, devices = env.layers, env.devices
    ring = Ring(devices, env.x_in.shape[1], env.send_sems, env.recv_sems)
    own = aligned(ring.me, ring.rows)
    blocks = []
    for layer in range(layers):
        blocks += [AttentionBlock(env, layer), MlpBlock(env, layer)]

    def load(block):
        copies = [pltpu.make_async_copy(src, dst, env.load_sems.at[block.load_base + index])
                  for index, (src, dst) in enumerate(block.loads)]
        for copy in copies:
            copy.start()
        return copies

    stores = {}
    loads = {block: load(block) for block in blocks[:2]}

    def need(block):
        for copy in loads.pop(block, ()):
            copy.wait()

    def store(block, indices):
        for index in indices:
            src, dst = block.weights[index]
            copy = pltpu.make_async_copy(src, dst.at[block.layer], env.store_sems.at[block.sems[index]])
            copy.start()
            stores.setdefault(block, []).append(copy)

    barrier = pltpu.get_barrier_semaphore()
    others = [lax.rem(ring.me + step, devices) for step in range(1, devices)]
    for peer in others:
        pl.semaphore_signal(barrier, inc=1, device_id={'tp': peer}, device_id_type=MESH)
    pl.semaphore_wait(barrier, len(others))

    uses = []

    def full_start(block, micro):
        if uses:
            pl.semaphore_wait(env.credit, len(ring.peers))
        uses.append(block)
        env.full[own, :] = norm_rows(block.rows_ref[micro], block.gain)
        ring.used = 0
        gather = Gather(ring, env.full)
        gather.start()
        ring.used = AG_COPIES
        return gather

    def resume(index):
        ring.used = index

    total_uses = 4 * len(blocks) - 1

    def full_done(gather):
        gather.sent()
        if len(uses) < total_uses:
            for peer in ring.peers:
                pl.semaphore_signal(env.credit, inc=1, device_id={'tp': peer}, device_id_type=MESH)

    def gather_base(micro):
        return AG_COPIES * (1 + micro)

    def reduce_base(micro):
        return AG_COPIES * 3 + RS_COPIES * HALVES * micro

    def staged(base, start, step):
        resume(base + start)
        return step()

    def relay(gather, base):
        staged(base, 5, gather.relay)

    def finish(gather, base):
        staged(base, 9, gather.finish)

    reducers = [None, None]

    def reduce_start(micro, partial):
        reducers[micro] = []
        for half in range(HALVES):
            partial(micro, half)
            reducer = Reduce(ring, env.part.at[micro, half], tuple(buf.at[micro, half] for buf in (
                env.from_partner, env.sums, env.via_left, env.via_right, env.in_left, env.in_right)))
            reducers[micro].append(reducer)
            staged(reduce_base(micro) + RS_COPIES * half, 0, reducer.start)

    def reduce_far(micro):
        for half, reducer in enumerate(reducers[micro]):
            staged(reduce_base(micro) + RS_COPIES * half, 4, reducer.far_out)

    def reduce_near(micro):
        for half, reducer in enumerate(reducers[micro]):
            staged(reduce_base(micro) + RS_COPIES * half, 6, reducer.near_out)

    def reduce_relay(micro):
        for half, reducer in enumerate(reducers[micro]):
            staged(reduce_base(micro) + RS_COPIES * half, 8, reducer.relay)

    def reduce_finish(micro):
        reducer, = reducers[micro]
        total = reducer.finish()
        reducer.sent()
        reducers[micro] = None
        return total

    def after_forward(index, micro):
        total = reduce_finish(micro)
        block = blocks[index]
        rows = residual(block.rows_ref[micro], total)
        if index + 1 < len(blocks):
            blocks[index + 1].rows_ref[micro] = rows
        else:
            env.y_out[micro] = rows

    for micro in range(2):
        blocks[0].rows_ref[micro] = env.x_in[micro]
    back = blocks[::-1]
    cot_rows = env.cot_rows
    for micro in range(2):
        cot_rows[0, micro] = env.y_cot[micro]
    cot_gathers = [None, None]

    def cot_start(index, micro):
        cots = env.cots.at[index % 2, micro]
        cots[own, :] = cot_rows[index % 2, micro]
        resume(gather_base(micro))
        cot_gathers[micro] = Gather(ring, cots)
        cot_gathers[micro].start()

    gather = full_start(blocks[0], 0)
    relay(gather, 0)
    for index, block in enumerate(blocks):
        last = index + 1 == len(blocks)
        for micro in range(2):
            finish(gather, 0)
            need(block)
            block.gathered(micro)
            if not last or micro == 0:
                full_done(gather)
            for step in FORWARD_ORDER:
                if step == 'X':
                    block.forward(micro)
                    reduce_start(micro, block.forward_partial)
                elif step == 'E':
                    if micro == 0:
                        if index > 0:
                            after_forward(index - 1, 1)
                        gather = full_start(block, 1)
                    else:
                        if last:
                            cot_start(0, 1)
                        after_forward(index, 0)
                        if last:
                            cot_start(0, 0)
                        else:
                            gather = full_start(blocks[index + 1], 0)
                elif step == 'f':
                    reduce_far(micro)
                elif step == 'r':
                    if last and micro == 1:
                        relay(cot_gathers[1], gather_base(1))
                    else:
                        relay(gather, 0)
                elif step == 'n':
                    reduce_near(micro)
                else:
                    reduce_relay(micro)
        if index + 2 < len(blocks):
            loads[blocks[index + 2]] = load(blocks[index + 2])

    def after_backward(index, micro):
        block = back[index]
        unit, scale = norm_unit(block.rows_ref[micro])
        total = reduce_finish(micro).astype(BF16).astype(F32)
        rows = (cot_rows[index % 2, micro].astype(F32) + norm_rows_backward(unit, scale, block.gain, total)).astype(BF16)
        if index + 1 < len(back):
            cot_rows[(index + 1) % 2, micro] = rows
            cot_start(index + 1, micro)
        else:
            env.grad_x[micro] = rows
        gain_row = slice(block.gain_row, block.gain_row + 1)
        grad_gain = jnp.sum(total * unit, axis=0, keepdims=True)
        env.gains[gain_row, :] = grad_gain if micro == 1 else env.gains[gain_row, :] + grad_gain

    for index, block in enumerate(back):
        last = index + 1 == len(back)
        for second in (False, True):
            micro, other = (0, 1) if second else (1, 0)
            finish(cot_gathers[micro], gather_base(micro))
            if second or index > 0:
                finish(gather, 0)
            need(block)
            going = not second or not last
            for step in BACKWARD_ORDER:
                if step == 'X':
                    block.backward(micro, env.cots.at[index % 2, micro])
                elif step == 'P':
                    if index == 0 and not second:
                        after_forward(len(blocks) - 1, 1)
                        for peer in ring.peers:
                            pl.semaphore_signal(env.turn, inc=1, device_id={'tp': peer}, device_id_type=MESH)
                        pl.semaphore_wait(env.turn, len(ring.peers))
                    reduce_start(micro, block.backward_partial)
                elif step == 'E':
                    if second:
                        after_backward(index, 1)
                    elif index > 0:
                        after_backward(index - 1, 0)
                elif step == 'f':
                    reduce_far(micro)
                elif step == 'w':
                    store(block, block.weights_near(second))
                    full_done(gather)
                    cot_gathers[micro].sent()
                elif step == 'r':
                    if going:
                        relay(cot_gathers[other], gather_base(other))
                elif step == 'V':
                    if going:
                        gather = full_start(back[index + 1] if second else block, other)
                elif step == 'n':
                    reduce_near(micro)
                elif step == 'R':
                    reduce_relay(micro)
                elif step == 'v':
                    if going:
                        relay(gather, 0)
                elif second:
                    store(block, block.weights_far([env.cots.at[index % 2, 0], env.cots.at[index % 2, 1]]))
                elif index > 0 and not last:
                    for copy in stores.pop(back[index - 1], ()):
                        copy.wait()
                    loads[back[index + 1]] = load(back[index + 1])
    after_backward(len(back) - 1, 0)

    copies = []
    for index, peer in enumerate(others):
        copy = pltpu.make_async_remote_copy(env.gains, env.gain_parts.at[ring.me], env.gain_send.at[index],
                                            env.gain_recv.at[index], device_id={'tp': peer}, device_id_type=MESH)
        copy.start()
        copies.append(copy)
    env.gain_parts[ring.me] = env.gains[...]
    for copy in copies:
        copy.wait()
    total = env.gain_parts[0]
    for index in range(1, devices):
        total = total + env.gain_parts[index]
    env.gain_out[...] = total
    for copies in stores.values():
        for copy in copies:
            copy.wait()


def comm_params(collective_id):
    return pltpu.CompilerParams(collective_id=collective_id, has_side_effects=True, vmem_limit_bytes=66_000_000)


def solution(mesh):
    devices = mesh.shape['tp']
    row_spec = P(None, ('dp', 'tp'), None)
    gain_spec = P(None, None)
    qkv_spec = P(None, None, 'tp', None, None)
    head_spec = P(None, 'tp', None, None)
    col_spec = P(None, None, 'tp')
    row_shard_spec = P(None, 'tp', None)

    def device_program(x_in, y_cot, gain_attn, gain_mlp, w_qkv, w_out, w_gate, w_up, w_down):
        micros, rows, width = x_in.shape
        layers = w_qkv.shape[0]
        groups = w_qkv.shape[3] - 2
        head_dim = w_qkv.shape[4]
        seq_len = rows * devices
        qkv_width = (groups + 2) * head_dim
        mix_width = groups * head_dim
        inner_width = w_gate.shape[2]
        inputs = {
            'x_in': (x_in, VMEM), 'y_cot': (y_cot, VMEM), 'gain_attn': (gain_attn, VMEM), 'gain_mlp': (gain_mlp, VMEM),
            'w_qkv': (w_qkv.reshape(layers, width, qkv_width), ANY), 'w_out': (w_out.reshape(layers, mix_width, width), ANY),
            'w_gate': (w_gate, ANY), 'w_up': (w_up, ANY), 'w_down': (w_down, ANY)}

        def out(shape, dtype, spec):
            return jax.ShapeDtypeStruct(shape, dtype), spec

        outputs = {
            'y_out': out(x_in.shape, BF16, VMEM), 'grad_x': out(x_in.shape, BF16, VMEM),
            'grad_qkv_out': out((layers, width, qkv_width), BF16, ANY), 'grad_out_out': out((layers, mix_width, width), BF16, ANY),
            'grad_gate_out': out(w_gate.shape, BF16, ANY), 'grad_up_out': out(w_up.shape, BF16, ANY),
            'grad_down_out': out(w_down.shape, BF16, ANY), 'gain_out': out((2 * layers, width), F32, VMEM)}

        def bf16(*shape):
            return pltpu.VMEM(shape, BF16)

        def f32(*shape):
            return pltpu.VMEM(shape, F32)

        def dma(count):
            return pltpu.SemaphoreType.DMA((count,))

        copies = 3 * AG_COPIES + 2 * HALVES * RS_COPIES
        scratch = {
            'layer_rows': bf16(layers, micros, rows, width), 'hidden_rows': bf16(layers, micros, rows, width),
            'cot_rows': bf16(2, micros, rows, width), 'qkv': bf16(layers, micros, seq_len, qkv_width),
            'mix': bf16(layers, micros, seq_len, mix_width), 'inner': bf16(micros, seq_len, inner_width),
            'grad_gate': bf16(seq_len, inner_width), 'grad_up': bf16(seq_len, inner_width),
            'grad_mix': bf16(seq_len, mix_width), 'grad_qkv': bf16(seq_len, qkv_width),
            'qkv_w': bf16(width, qkv_width), 'out_w': bf16(mix_width, width), 'gate_w': bf16(width, inner_width),
            'up_w': bf16(width, inner_width), 'down_w': bf16(inner_width, width),
            'stage_qkv': bf16(width, qkv_width), 'stage_gate': bf16(width, inner_width), 'stage_up': bf16(width, inner_width),
            'acc_qkv': f32(width, qkv_width), 'acc_gate': f32(width, inner_width), 'acc_up': f32(width, inner_width),
            'full': bf16(seq_len, width), 'cots': bf16(2, micros, seq_len, width), 'part': f32(micros, HALVES, seq_len, width // HALVES),
            'from_partner': f32(micros, HALVES, 4, rows, width // HALVES), 'sums': f32(micros, HALVES, 4, rows, width // HALVES),
            'via_left': f32(micros, HALVES, rows // 2, width // HALVES), 'via_right': f32(micros, HALVES, rows // 2, width // HALVES),
            'in_left': f32(micros, HALVES, rows, width // HALVES), 'in_right': f32(micros, HALVES, rows, width // HALVES),
            'gains': f32(2 * layers, width), 'gain_parts': f32(devices, 2 * layers, width),
            'load_sems': dma(5), 'store_sems': dma(5), 'send_sems': dma(copies), 'recv_sems': dma(copies),
            'gain_send': dma(devices - 1), 'gain_recv': dma(devices - 1), 'credit': pltpu.SemaphoreType.REGULAR, 'turn': pltpu.SemaphoreType.REGULAR}
        names = (*inputs, *outputs, *scratch)
        sizes = dict(layers=layers, devices=devices, groups=groups, head_dim=head_dim)
        results = pl.pallas_call(
            functools.partial(stack_kernel, names, sizes),
            out_shape=tuple(shape for shape, spec in outputs.values()),
            in_specs=[spec for array, spec in inputs.values()], out_specs=tuple(spec for shape, spec in outputs.values()),
            scratch_shapes=list(scratch.values()), compiler_params=comm_params(0), name='stack',
        )(*(array for array, spec in inputs.values()))
        y_rows, grad_rows, grad_qkv, grad_out, grad_gate, grad_up, grad_down, gain_sum = results
        return (y_rows, grad_rows, grad_qkv.reshape(w_qkv.shape), grad_out.reshape(w_out.shape), grad_gate, grad_up, grad_down,
                gain_sum[:layers], gain_sum[layers:])

    return jax.shard_map(device_program, mesh=mesh,
                         in_specs=(row_spec, row_spec, gain_spec, gain_spec, qkv_spec, head_spec, col_spec, col_spec, row_shard_spec),
                         out_specs=(row_spec, row_spec, P('dp', None, 'tp', None, None), P('dp', 'tp', None, None), P('dp', None, 'tp'), P('dp', None, 'tp'), P('dp', 'tp', None), P('dp', None), P('dp', None)),
                         check_vma=False)
```
